32 devices in a mesh: seq: 16 (over z, y, x), tp: 2 (over core).
Axes of the slice: x: 2, y: 2, z: 4, core: 2. Of those that a mesh axis runs over, the one named last changes fastest.
Arguments:
- inner_input: bfloat16 [4096, 2560], P('seq', 'tp'), may hold values from -6 to 6
- gate_input: bfloat16 [4096, 2560], P('seq', 'tp'), may hold values from -170 to 170
- state_input: bfloat16 [4096, 256], P('seq'), may hold values from -6 to 6
- step_raw: float32 [40, 4096], P('tp', 'seq'), may hold values from -14 to 0
- conv_inner: float32 [4, 2560], P(None, 'tp'), may hold values from -3 to 3
- conv_state: float32 [4, 256], replicated, may hold values from -3 to 3
- bias_inner: float32 [2560], P('tp'), may hold values from -3 to 3
- bias_state: float32 [256], replicated, may hold values from -3 to 3
- step_bias: float32 [40], P('tp'), may hold values from -0.3 to 0.3
- decay_log: float32 [40], P('tp'), may hold values from -1.4 to 0
- skip_gain: float32 [40], P('tp'), may hold values from 0.5 to 1.5
- norm_gain: float32 [2560], P('tp'), may hold values from 0.1 to 1.9
- out_weight: bfloat16 [2560, 2560], P('tp'), may hold values from -0.15625 to 0.15625
Outputs:
- block_out: bfloat16 [4096, 2560], P('seq', 'tp')
The draws below stay inside these ranges and needn't reach their ends.
All inputs are finite; a program needn't handle non-finite values.
Results may differ from the reference program's by a relative error of at most 0.008.
Values may be sent and summed in bfloat16 or wider, within the bound.
A program may use at most 64 MiB of HBM per device.

```python
import math
import jax
import jax.numpy as jnp
from jax import lax

D = 2560
HEADS = 40
HEAD_DIM = 64
NSTATE = 128
KW = 4
INNER = 2560
TOKEN_COUNT = 4096


def draw_gate_input(key, part):
    second = jax.random.fold_in(key, 1)
    columns = jnp.arange(INNER, dtype=jnp.float32) / INNER
    values = jnp.clip(jax.random.normal(second, (TOKEN_COUNT, INNER)), -5.0, 5.0)
    return (values * jnp.exp(jnp.log(3.0) * columns)[None, :]).astype(jnp.bfloat16)


def draw_step_raw(key, part):
    random_keys = jax.random.split(key, 4)
    share = 0.5
    slow_heads = jax.random.uniform(random_keys[0], (HEADS,)) < share
    base_step = jnp.exp(jax.random.uniform(random_keys[1], (HEADS,), minval=jnp.log(0.05), maxval=jnp.log(0.2)))
    jitter_amount = jnp.exp(jax.random.uniform(random_keys[2], (HEADS, TOKEN_COUNT), minval=-0.7, maxval=0.7))
    spike_points = jax.random.randint(random_keys[3], (4,), 0, TOKEN_COUNT)
    at_spike_point = jnp.any(jnp.arange(TOKEN_COUNT)[None, :] == spike_points[:, None], axis=0)
    gentle_step = jnp.where(at_spike_point[None, :], 0.25, jitter_amount / TOKEN_COUNT)
    target = jnp.where(slow_heads[:, None], gentle_step, base_step[:, None] * jitter_amount)
    return jnp.log(jnp.expm1(target)).astype(jnp.float32)


def with_spikes(result, key, source, target, shards_of, factor):
    owner, partner = [(jnp.arange(result.shape[dim]) // (result.shape[dim] // shards_of)).reshape([-1 if axis == dim else 1 for axis in range(result.ndim)]) for dim in (source, target)]
    chosen = jax.random.permutation(key, shards_of)[partner]
    strong = (owner == chosen) | (owner == (partner + shards_of // 2) % shards_of)
    return jnp.where(strong, factor * result, result)


def block_levels(stream_key, dims, cuts, low, largest):
    loudness, own = 1.0, jax.random.fold_in(stream_key, 6)
    for dim, parts in cuts:
        draws = jnp.exp(jax.random.uniform(jax.random.fold_in(own, dim), (parts,), jnp.float32, low / len(cuts), largest / len(cuts)))
        loudness = loudness * jnp.repeat(draws, dims[dim] // parts).reshape([-1 if axis == dim else 1 for axis in range(len(dims))])
    return loudness


def scatter_about(stream_key, shape, scale, most, shards=(), kind=jnp.bfloat16):
    array = jax.random.normal(stream_key, shape, jnp.float32) * scale
    if len(shards) > 0:
        array = block_levels(stream_key, shape, shards, -0.22, 0.18) * array
    return jnp.clip(array, min=-most, max=most).astype(kind)


def heavy_noise(stream_key, shape, width, most, cuts, heavy, kind=jnp.bfloat16):
    array = width * jax.random.normal(stream_key, shape, jnp.float32)
    if cuts:
        array = array * block_levels(stream_key, shape, cuts, -0.22, 0.18)
    return jnp.clip(with_spikes(array, jax.random.fold_in(stream_key, 3), *heavy), -most, most).astype(kind)


def setup_inputs(seed: int = 0) -> dict:
    seeds = jax.random.split(jax.random.key(seed), 14)
    return {
        "inner_input": scatter_about(seeds[0], (TOKEN_COUNT, INNER), 1.0, 6.0, ((0, 16), (1, 2))),
        "gate_input": draw_gate_input(jax.random.fold_in(seeds[13], 71), 0),
        "state_input": scatter_about(seeds[2], (TOKEN_COUNT, 2 * NSTATE), 1.0, 6.0, ((0, 16),)),
        "step_raw": draw_step_raw(jax.random.fold_in(seeds[13], 71), 0),
        "conv_inner": scatter_about(seeds[4], (KW, INNER), KW ** -0.5, 3.0, ((1, 2),), jnp.float32),
        "conv_state": scatter_about(seeds[5], (KW, 2 * NSTATE), KW ** -0.5, 3.0, (), jnp.float32),
        "bias_inner": scatter_about(seeds[6], (INNER,), 0.5, 3.0, ((0, 2),), jnp.float32),
        "bias_state": scatter_about(seeds[7], (2 * NSTATE,), 0.5, 3.0, (), jnp.float32),
        "step_bias": jnp.clip(jax.random.uniform(seeds[8], (HEADS,), jnp.float32, -0.3, 0.3) * block_levels(seeds[8], (HEADS,), ((0, 2),), -0.4, 0.0), -0.3, 0.3),
        "decay_log": jnp.clip(-1.4 + 1.4 * jax.random.uniform(seeds[9], (HEADS,), jnp.float32) ** block_levels(seeds[9], (HEADS,), ((0, 2),), -0.2, 0.2), -1.4, 0.0),
        "skip_gain": jnp.clip(0.5 + 1.0 * jax.random.uniform(seeds[10], (HEADS,), jnp.float32) ** block_levels(seeds[10], (HEADS,), ((0, 2),), -0.2, 0.2), 0.5, 1.5),
        "norm_gain": jnp.clip(1.0 + 0.18 * jax.random.normal(seeds[11], (INNER,), jnp.float32), 0.1, 1.9),
        "out_weight": heavy_noise(seeds[12], (INNER, D), INNER ** -0.5, 0.15625, ((0, 2),), (0, 1, 2, 2.0)),
    }


highest = lax.Precision.HIGHEST

def conv_silu(padded, weights, offsets, length):
    width_taps = weights.shape[0]
    summed = offsets.astype(jnp.float32)[None, :] + jnp.zeros((length, weights.shape[1]), jnp.float32)
    for number in range(width_taps):
        summed = summed + weights[number][None, :] * padded[number:number + length]
    return jax.nn.silu(summed).astype(jnp.bfloat16)

def block_step(state_now, pieces):
    inner_rows, keys_b, query_c, step_sizes, log_decay = pieces
    cumulative = jnp.cumsum(log_decay, axis=1)
    block_rows = log_decay.shape[1]
    causal = jnp.arange(block_rows)[:, None] >= jnp.arange(block_rows)[None, :]
    spread = jnp.where(causal[None], cumulative[:, :, None] - cumulative[:, None, :], -jnp.inf)
    scores = jnp.dot(query_c, keys_b.T, precision=highest)
    weights = scores[None] * jnp.exp(spread) * step_sizes[:, None, :]
    output = jnp.einsum('hts,shp->thp', weights, inner_rows, precision=highest)
    carried = jnp.einsum('tn,hnp->thp', query_c, state_now, precision=highest)
    output = output + carried * jnp.exp(cumulative).T[:, :, None]
    towards_end = jnp.exp(cumulative[:, -1:] - cumulative) * step_sizes
    update = jnp.einsum('sn,shp->hnp', keys_b, inner_rows * towards_end.T[:, :, None], precision=highest)
    state_next = jnp.exp(cumulative[:, -1])[:, None, None] * state_now + update
    return (state_next, output)

def reference(inner_input, gate_input, state_input, step_raw, conv_inner, conv_state, bias_inner, bias_state, step_bias, decay_log, skip_gain, norm_gain, out_weight):
    width_taps = conv_inner.shape[0]
    pad_rows = ((width_taps - 1, 0), (0, 0))
    inner_conv = conv_silu(jnp.pad(inner_input.astype(jnp.float32), pad_rows), conv_inner, bias_inner, TOKEN_COUNT)
    state_conv = conv_silu(jnp.pad(state_input.astype(jnp.float32), pad_rows), conv_state, bias_state, TOKEN_COUNT)
    step_sizes = jax.nn.softplus(step_raw + step_bias[:, None])
    log_decay = -jnp.exp(decay_log)[:, None] * step_sizes
    block_size = math.gcd(TOKEN_COUNT, 256)
    blocks = TOKEN_COUNT // block_size
    inner_float = inner_conv.astype(jnp.float32)
    inner_rows = inner_float.reshape(blocks, block_size, HEADS, HEAD_DIM)
    keys_b = state_conv[:, :NSTATE].astype(jnp.float32).reshape(blocks, block_size, NSTATE)
    query_c = state_conv[:, NSTATE:].astype(jnp.float32).reshape(blocks, block_size, NSTATE)
    step_block_grid = step_sizes.reshape(HEADS, blocks, block_size).transpose(1, 0, 2)
    log_blocks = log_decay.reshape(HEADS, blocks, block_size).transpose(1, 0, 2)
    start_state = jnp.zeros((HEADS, NSTATE, HEAD_DIM), jnp.float32)
    final_state, outputs = lax.scan(block_step, start_state, (inner_rows, keys_b, query_c, step_block_grid, log_blocks))
    mixed = outputs.reshape(TOKEN_COUNT, HEADS, HEAD_DIM) + skip_gain[None, :, None] * inner_float.reshape(TOKEN_COUNT, HEADS, HEAD_DIM)
    gated_raw = mixed.reshape(TOKEN_COUNT, INNER) * jax.nn.silu(gate_input.astype(jnp.float32))
    squares = lax.optimization_barrier(jnp.sum(gated_raw * gated_raw, axis=1))
    scale_inv = lax.rsqrt(squares / INNER + 1e-05)
    gated = (gated_raw * norm_gain[None, :]).astype(jnp.bfloat16)
    summed = jnp.dot(gated, out_weight, preferred_element_type=jnp.float32)
    return (summed * scale_inv[:, None]).astype(jnp.bfloat16)
```

```python
import functools

import jax
import jax.numpy as jnp
from jax import lax
from jax.experimental import pallas as pl
from jax.experimental.pallas import tpu as pltpu
from jax.sharding import PartitionSpec as P

HEAD_DIM = 64
NSTATE = 128
LANES = 128
GROUP = 32
RIM = 8
MESH = pl.DeviceIdType.MESH
f32 = jnp.float32
bf16 = jnp.bfloat16


def silu(v):
    return v / (1.0 + jnp.exp(-v))


def log1p_exp(v):
    u = jnp.exp(-jnp.abs(v))
    z = u / (2.0 + u)
    q = z * z
    series = jnp.full_like(q, 1.0 / 19.0)
    for odd in range(17, 0, -2):
        series = series * q + 1.0 / odd
    return jnp.maximum(v, 0.0) + 2.0 * z * series


def spread_heads(table, ones):
    high = table.astype(bf16)
    low = (table - high.astype(f32)).astype(bf16)
    out = jnp.dot(high, ones, preferred_element_type=f32)
    return out + jnp.dot(low, ones, preferred_element_type=f32)


def conv_rows(src, taps, bias, start, rows, columns):
    count = taps.shape[0]
    total = bias[...]
    for k in range(count):
        first = start + RIM - count + 1 + k
        total = total + taps[k : k + 1] * src[pl.ds(first, rows), columns]
    return silu(total)


def kernel(
    n,
    x_hbm, gate_hbm, state_in, step_raw, taps_x, taps_s, bias_x, bias_s,
    step_bias, decay_log, skip_gain, norm_gain, w_hbm,
    out_ref,
    x_in, gate_in, w_all, x_pad, s_pad, x_conv, s_conv, table, spread, cols,
    scores, mixed, gate_act, decayed, gated,
    rim_x, rim_s, decay_out, decay_all, decay_cols,
    full, slices, got1, back, got2, entering,
    part, part_got, own, squares, squares_got,
    load_sem, rim_send, rim_recv, d_send, d_recv, s1_send, s1_recv,
    s2_send, s2_recv, o_send, o_recv, q_sem,
):
    me = lax.axis_index("seq")
    core = lax.axis_index("tp")
    other = 1 - core
    rows, inner = x_in.shape
    heads = step_raw.shape[0]
    tiles = inner // LANES
    per = NSTATE // n
    slot = slices.shape[1]
    half = rows // 2

    barrier = pltpu.get_barrier_semaphore()

    def greet(k, _):
        pl.semaphore_signal(
            barrier, inc=1, device_id={"seq": lax.rem(me + k, n)}, device_id_type=MESH
        )
        return 0

    lax.fori_loop(1, n, greet, 0)
    pl.semaphore_signal(barrier, inc=1, device_id={"tp": other}, device_id_type=MESH)

    load_x = pltpu.make_async_copy(x_hbm, x_in, load_sem.at[0])
    load_g = pltpu.make_async_copy(gate_hbm, gate_in, load_sem.at[1])
    load_w = pltpu.make_async_copy(w_hbm, w_all, load_sem.at[2])
    load_x.start()
    load_g.start()
    load_w.start()

    eye = (
        lax.broadcasted_iota(jnp.int32, (heads, heads), 0)
        == lax.broadcasted_iota(jnp.int32, (heads, heads), 1)
    )

    def as_column(row):
        return jnp.sum(jnp.where(eye, row[...], 0.0), axis=1, keepdims=True)

    step = log1p_exp(step_raw[...] + as_column(step_bias))
    log_decay = -jnp.exp(as_column(decay_log)) * step
    upper = (
        lax.broadcasted_iota(jnp.int32, (rows, rows), 0)
        <= lax.broadcasted_iota(jnp.int32, (rows, rows), 1)
    ).astype(f32)
    cum = jnp.dot(
        log_decay, upper, precision=lax.Precision.HIGHEST, preferred_element_type=f32
    )
    shifted = cum - jnp.log(step)
    table[...] = jnp.zeros_like(table)
    table[0:heads] = cum
    table[GROUP : GROUP + heads] = jnp.exp(cum[:, rows - 1 : rows] - shifted)
    table[2 * GROUP : 2 * GROUP + heads] = jnp.exp(cum)
    flipped = table[...].T
    cols[...] = flipped
    lane = lax.broadcasted_iota(jnp.int32, (1, LANES), 1) // GROUP
    decay_out[...] = jnp.where(
        lane == 2, jnp.broadcast_to(flipped[rows - 1 : rows], (8, LANES)), 0.0
    )
    decay_all[me] = decay_out[...]

    pl.semaphore_wait(barrier, n)

    def rim_copies():
        target = {"seq": lax.rem(me + 1, n)}
        return [
            pltpu.make_async_remote_copy(
                src_ref=src.at[pl.ds(rows - RIM, RIM)],
                dst_ref=dst,
                send_sem=rim_send.at[i],
                recv_sem=rim_recv.at[i],
                device_id=target,
                device_id_type=MESH,
            )
            for i, (src, dst) in enumerate(((x_hbm, rim_x), (state_in, rim_s)))
        ]

    @pl.when(me < n - 1)
    def _():
        for copy in rim_copies():
            copy.start()

    def decay_copy(k):
        to = lax.rem(me + k, n)
        return pltpu.make_async_remote_copy(
            src_ref=decay_out,
            dst_ref=decay_all.at[me],
            send_sem=d_send.at[k],
            recv_sem=d_recv.at[me],
            device_id={"seq": to},
            device_id_type=MESH,
        )

    def decay_start(k, _):
        decay_copy(k).start()
        return 0

    lax.fori_loop(1, n, decay_start, 0)

    spread[...] = jnp.where(
        lax.broadcasted_iota(jnp.int32, (LANES, inner), 0) % GROUP
        == lax.broadcasted_iota(jnp.int32, (LANES, inner), 1) // HEAD_DIM,
        1.0,
        0.0,
    ).astype(bf16)

    s_pad[0:RIM] = jnp.zeros((RIM, s_pad.shape[1]), f32)
    s_pad[RIM:] = state_in[...].astype(f32)
    s_conv[...] = conv_rows(s_pad, taps_s, bias_s, 0, rows, slice(None)).astype(bf16)
    x_pad[0:RIM] = jnp.zeros((RIM, inner), f32)
    load_x.wait()
    for i in range(tiles):
        c = slice(i * LANES, (i + 1) * LANES)
        x_pad[RIM:, c] = x_in[:, c].astype(f32)
        x_conv[:, c] = conv_rows(
            x_pad, taps_x[:, c], bias_x[:, c], 0, rows, c
        ).astype(bf16)

    @pl.when(me > 0)
    def _():
        for copy in rim_copies():
            copy.wait_recv()
        s_pad[0:RIM] = rim_s[...].astype(f32)
        x_pad[0:RIM] = rim_x[...].astype(f32)

    s_conv[0:16] = conv_rows(s_pad, taps_s, bias_s, 0, 16, slice(None)).astype(bf16)
    x_conv[0:16] = conv_rows(x_pad, taps_x, bias_x, 0, 16, slice(None)).astype(bf16)

    towards = jnp.where(lane == 1, cols[...], 0.0)
    for i in range(tiles):
        c = slice(i * LANES, (i + 1) * LANES)
        scaled = (
            x_conv[:, c].astype(f32) * spread_heads(towards, spread[:, c])
        ).astype(bf16)
        full[:, c] = lax.dot_general(
            s_conv[:, :NSTATE], scaled, (((0,), (0,)), ((), ())),
            preferred_element_type=f32,
        )

    def cut(j, _):
        piece = full[pl.ds(pl.multiple_of(j * per, per), per), :]
        slices[j] = jnp.broadcast_to(piece, (slot, inner)).astype(bf16)
        return 0

    lax.fori_loop(0, n, cut, 0)

    def state_copy(k):
        to = lax.rem(me + k, n)
        return pltpu.make_async_remote_copy(
            src_ref=slices.at[to],
            dst_ref=got1.at[me],
            send_sem=s1_send.at[k],
            recv_sem=s1_recv.at[me],
            device_id={"seq": to},
            device_id_type=MESH,
        )

    @pl.when(me < n - 1)
    def _():
        def start(k, _):
            state_copy(k).start()
            return 0

        lax.fori_loop(1, n, start, 0)

    got1[me] = slices[me]

    def decay_wait(k, _):
        source = lax.rem(me + k, n)
        pltpu.make_async_remote_copy(
            src_ref=decay_out,
            dst_ref=decay_all.at[source],
            send_sem=d_send.at[k],
            recv_sem=d_recv.at[source],
            device_id={"seq": source},
            device_id_type=MESH,
        ).wait_recv()
        return 0

    lax.fori_loop(1, n, decay_wait, 0)
    decay_cols[...] = spread_heads(
        decay_all[...].reshape(n * 8, LANES), spread[...]
    ).reshape(n, 8, inner)

    keys = s_conv[:, :NSTATE]
    query = s_conv[:, NSTATE:]
    causal = (
        lax.broadcasted_iota(jnp.int32, (rows, rows), 0)
        >= lax.broadcasted_iota(jnp.int32, (rows, rows), 1)
    )
    scores[...] = jnp.where(
        causal,
        lax.dot_general(
            query, keys, (((1,), (1,)), ((), ())), preferred_element_type=f32
        ),
        0.0,
    )
    first_half = lax.broadcasted_iota(jnp.int32, (1, LANES), 1) < HEAD_DIM

    def inside(i):
        c = slice(i * LANES, (i + 1) * LANES)
        x_c = x_conv[:, c]
        tops, bottoms = [], []
        for h in (2 * i, 2 * i + 1):
            a_row = shifted[h : h + 1, :]
            top = cols[0:half, h : h + 1] - a_row[:, :half]
            top = scores[0:half, 0:half] * jnp.exp(jnp.minimum(top, 80.0))
            tops.append(
                jnp.dot(top.astype(bf16), x_c[:half], preferred_element_type=f32)
            )
            low = cols[half:, h : h + 1] - a_row
            low = scores[half:, :] * jnp.exp(jnp.minimum(low, 80.0))
            bottoms.append(jnp.dot(low.astype(bf16), x_c, preferred_element_type=f32))
        gain = jnp.where(
            first_half,
            skip_gain[:, 2 * i : 2 * i + 1],
            skip_gain[:, 2 * i + 1 : 2 * i + 2],
        )
        x_f = x_c.astype(f32)
        mixed[0:half, c] = jnp.where(first_half, *tops) + gain * x_f[:half]
        mixed[half:, c] = jnp.where(first_half, *bottoms) + gain * x_f[half:]

    split = (tiles * 6) // 10
    for i in range(split):
        inside(i)

    state = jnp.zeros((slot, inner), f32)

    def prefix(j, state):
        back[j] = state.astype(bf16)

        @pl.when(j != me)
        def _():
            pltpu.make_async_remote_copy(
                src_ref=slices.at[j],
                dst_ref=got1.at[j],
                send_sem=s1_send.at[0],
                recv_sem=s1_recv.at[j],
                device_id={"seq": lax.rem(me + 1, n)},
                device_id_type=MESH,
            ).wait_recv()

        return decay_cols[j][0:1] * state + got1[j].astype(f32)

    state = lax.fori_loop(0, n - 1, prefix, state)
    back[n - 1] = state.astype(bf16)

    def back_copy(k):
        to = lax.rem(me + k, n)
        return to, pltpu.make_async_remote_copy(
            src_ref=back.at[to],
            dst_ref=got2.at[me],
            send_sem=s2_send.at[k],
            recv_sem=s2_recv.at[me],
            device_id={"seq": to},
            device_id_type=MESH,
        )

    def back_start(k, _):
        to, copy = back_copy(k)

        @pl.when(to > 0)
        def _():
            copy.start()

        return 0

    lax.fori_loop(1, n, back_start, 0)
    got2[me] = back[me]

    for i in range(split, tiles):
        inside(i)

    load_g.wait()
    carry_decay = jnp.where(lane == 2, cols[...], 0.0)
    for i in range(tiles):
        c = slice(i * LANES, (i + 1) * LANES)
        gate_act[:, c] = silu(gate_in[:, c].astype(f32))
        decayed[:, c] = spread_heads(carry_decay, spread[:, c])

    @pl.when(me > 0)
    def _():
        def back_wait(k, _):
            source = lax.rem(me + k, n)
            pltpu.make_async_remote_copy(
                src_ref=back.at[source],
                dst_ref=got2.at[source],
                send_sem=s2_send.at[k],
                recv_sem=s2_recv.at[source],
                device_id={"seq": source},
                device_id_type=MESH,
            ).wait_recv()
            return 0

        lax.fori_loop(1, n, back_wait, 0)

        def place(j, _):
            entering[pl.ds(pl.multiple_of(j * per, per), per), :] = got2[j].astype(
                f32
            )[0:per]
            return 0

        lax.fori_loop(0, n, place, 0)

    @pl.when(me == 0)
    def _():
        entering[...] = jnp.zeros_like(entering)

    total = jnp.zeros((rows, LANES), f32)
    for i in range(tiles):
        c = slice(i * LANES, (i + 1) * LANES)
        carried = jnp.dot(
            query, entering[:, c].astype(bf16), preferred_element_type=f32
        )
        raw = (mixed[:, c] + carried * decayed[:, c]) * gate_act[:, c]
        total = total + raw * raw
        gated[:, c] = (raw * norm_gain[:, c]).astype(bf16)
    squares[...] = total

    def across(src, dst, send, recv):
        return pltpu.make_async_remote_copy(
            src_ref=src,
            dst_ref=dst,
            send_sem=send,
            recv_sem=recv,
            device_id={"tp": other},
            device_id_type=MESH,
        )

    copy_q = across(squares, squares_got, q_sem.at[0], q_sem.at[1])
    copy_q.start()
    load_w.wait()
    pieces, _, width = part.shape

    def part_copy(p):
        return across(part.at[p], part_got.at[p], o_send.at[p], o_recv.at[p])

    for p in range(pieces):
        at = pl.ds(pl.multiple_of(other * inner + p * width, LANES), width)
        part[p] = jnp.dot(
            gated[...], w_all[:, at], preferred_element_type=f32
        ).astype(bf16)
        part_copy(p).start()
    for p in range(pieces):
        at = pl.ds(pl.multiple_of(core * inner + p * width, LANES), width)
        own[p] = jnp.dot(gated[...], w_all[:, at], preferred_element_type=f32)
    copy_q.wait_recv()
    both = jnp.sum(squares[...] + squares_got[...], axis=1, keepdims=True)
    scale = lax.rsqrt(both / (2 * inner) + 1e-05)
    for p in range(pieces):
        part_copy(p).wait_recv()
        out_ref[:, p * width : (p + 1) * width] = (
            (own[p] + part_got[p].astype(f32)) * scale
        ).astype(bf16)

    copy_q.wait_send()
    for p in range(pieces):
        part_copy(p).wait_send()

    def drain(k, _):
        decay_copy(k).wait_send()
        to, copy = back_copy(k)

        @pl.when(to > 0)
        def _():
            copy.wait_send()

        return 0

    lax.fori_loop(1, n, drain, 0)

    @pl.when(me < n - 1)
    def _():
        for copy in rim_copies():
            copy.wait_send()

        def drain1(k, _):
            state_copy(k).wait_send()
            return 0

        lax.fori_loop(1, n, drain1, 0)


def local(
    inner_input, gate_input, state_input, step_raw, conv_inner, conv_state,
    bias_inner, bias_state, step_bias, decay_log, skip_gain, norm_gain, out_weight,
):
    n = lax.axis_size("seq")
    rows, inner = inner_input.shape
    maps = state_input.shape[1]
    slot = max(8, NSTATE // n)
    width = 256
    pieces = inner // width
    vm = pltpu.VMEM
    dma = pltpu.SemaphoreType.DMA
    any_spec = pl.BlockSpec(memory_space=pl.ANY)
    vmem_spec = pl.BlockSpec(memory_space=pltpu.VMEM)
    scratch = [
        vm((rows, inner), bf16),
        vm((rows, inner), bf16),
        vm(out_weight.shape, bf16),
        vm((rows + RIM, inner), f32),
        vm((rows + RIM, maps), f32),
        vm((rows, inner), bf16),
        vm((rows, maps), bf16),
        vm((LANES, rows), f32),
        vm((LANES, inner), bf16),
        vm((rows, LANES), f32),
        vm((rows, rows), f32),
        vm((rows, inner), f32),
        vm((rows, inner), f32),
        vm((rows, inner), f32),
        vm((rows, inner), bf16),
        vm((RIM, inner), bf16),
        vm((RIM, maps), bf16),
        vm((8, LANES), f32),
        vm((n, 8, LANES), f32),
        vm((n, 8, inner), f32),
        vm((NSTATE, inner), f32),
        vm((n, slot, inner), bf16),
        vm((n, slot, inner), bf16),
        vm((n, slot, inner), bf16),
        vm((n, slot, inner), bf16),
        vm((NSTATE, inner), f32),
        vm((pieces, rows, width), bf16),
        vm((pieces, rows, width), bf16),
        vm((pieces, rows, width), f32),
        vm((rows, LANES), f32),
        vm((rows, LANES), f32),
        dma((3,)), dma((2,)), dma((2,)),
        dma((n,)), dma((n,)), dma((n,)), dma((n,)), dma((n,)), dma((n,)),
        dma((pieces,)), dma((pieces,)), dma((2,)),
    ]
    row = lambda v: v.reshape(1, -1)
    return pl.pallas_call(
        functools.partial(kernel, n),
        out_shape=jax.ShapeDtypeStruct((rows, inner), bf16),
        in_specs=[any_spec, any_spec] + [vmem_spec] * 10 + [any_spec],
        out_specs=vmem_spec,
        scratch_shapes=scratch,
        compiler_params=pltpu.CompilerParams(
            collective_id=0, has_side_effects=True, vmem_limit_bytes=60 * 2**20
        ),
        name="ssd_block",
    )(
        inner_input, gate_input, state_input, step_raw, conv_inner, conv_state,
        row(bias_inner), row(bias_state), row(step_bias), row(decay_log),
        row(skip_gain), row(norm_gain), out_weight,
    )


def solution(mesh):
    return jax.shard_map(
        local,
        mesh=mesh,
        in_specs=(
            P("seq", "tp"),
            P("seq", "tp"),
            P("seq", None),
            P("tp", "seq"),
            P(None, "tp"),
            P(),
            P("tp"),
            P(),
            P("tp"),
            P("tp"),
            P("tp"),
            P("tp"),
            P("tp", None),
        ),
        out_specs=P("seq", "tp"),
        check_vma=False,
    )
```

```python
import functools

import jax
import jax.numpy as jnp
from jax import lax
from jax.experimental import pallas as pl
from jax.experimental.pallas import tpu as pltpu
from jax.sharding import PartitionSpec as P

HEAD_DIM = 64
NSTATE = 128
LANES = 128
GROUP = 32
RIM = 8
MESH = pl.DeviceIdType.MESH
f32 = jnp.float32
bf16 = jnp.bfloat16


def silu(v):
    return v / (1.0 + jnp.exp(-v))


def log1p_exp(v):
    u = jnp.exp(-jnp.abs(v))
    z = u / (2.0 + u)
    q = z * z
    series = jnp.full_like(q, 1.0 / 19.0)
    for odd in range(17, 0, -2):
        series = series * q + 1.0 / odd
    return jnp.maximum(v, 0.0) + 2.0 * z * series


def spread_heads(table, ones):
    high = table.astype(bf16)
    low = (table - high.astype(f32)).astype(bf16)
    out = jnp.dot(high, ones, preferred_element_type=f32)
    return out + jnp.dot(low, ones, preferred_element_type=f32)


def conv_rows(src, taps, bias, start, rows, columns):
    count = taps.shape[0]
    total = bias[...]
    for k in range(count):
        first = start + RIM - count + 1 + k
        total = total + taps[k : k + 1] * src[pl.ds(first, rows), columns]
    return silu(total)


def kernel(
    n,
    x_hbm, gate_hbm, state_in, step_raw, taps_x, taps_s, bias_x, bias_s,
    step_bias, decay_log, skip_gain, norm_gain, w_hbm,
    out_ref,
    x_in, gate_in, w_all, x_pad, s_pad, x_conv, s_conv, table, spread, cols,
    scores, mixed, gate_act, decayed, gated,
    rim_x, rim_s, decay_out, decay_all, decay_cols,
    full, slices, got1, back, got2, entering,
    part, part_got, own, squares, squares_got,
    load_sem, rim_send, rim_recv, d_send, d_recv, s1_send, s1_recv,
    s2_send, s2_recv, o_send, o_recv, q_sem,
):
    me = lax.axis_index("seq")
    core = lax.axis_index("tp")
    other = 1 - core
    rows, inner = x_in.shape
    heads = step_raw.shape[0]
    tiles = inner // LANES
    per = NSTATE // n
    slot = slices.shape[1]
    half = rows // 2

    barrier = pltpu.get_barrier_semaphore()

    def greet(k, _):
        pl.semaphore_signal(
            barrier, inc=1, device_id={"seq": lax.rem(me + k, n)}, device_id_type=MESH
        )
        return 0

    lax.fori_loop(1, n, greet, 0)
    pl.semaphore_signal(barrier, inc=1, device_id={"tp": other}, device_id_type=MESH)

    load_x = pltpu.make_async_copy(x_hbm, x_in, load_sem.at[0])
    load_g = pltpu.make_async_copy(gate_hbm, gate_in, load_sem.at[1])
    load_w = pltpu.make_async_copy(w_hbm, w_all, load_sem.at[2])
    load_x.start()
    load_g.start()
    load_w.start()

    eye = (
        lax.broadcasted_iota(jnp.int32, (heads, heads), 0)
        == lax.broadcasted_iota(jnp.int32, (heads, heads), 1)
    )

    def as_column(row):
        return jnp.sum(jnp.where(eye, row[...], 0.0), axis=1, keepdims=True)

    step = log1p_exp(step_raw[...] + as_column(step_bias))
    log_decay = -jnp.exp(as_column(decay_log)) * step
    upper = (
        lax.broadcasted_iota(jnp.int32, (rows, rows), 0)
        <= lax.broadcasted_iota(jnp.int32, (rows, rows), 1)
    ).astype(f32)
    cum = jnp.dot(
        log_decay, upper, precision=lax.Precision.HIGHEST, preferred_element_type=f32
    )
    shifted = cum - jnp.log(step)
    table[...] = jnp.zeros_like(table)
    table[0:heads] = cum
    table[GROUP : GROUP + heads] = jnp.exp(cum[:, rows - 1 : rows] - shifted)
    table[2 * GROUP : 2 * GROUP + heads] = jnp.exp(cum)
    flipped = table[...].T
    cols[...] = flipped
    lane = lax.broadcasted_iota(jnp.int32, (1, LANES), 1) // GROUP
    decay_out[...] = jnp.where(
        lane == 2, jnp.broadcast_to(flipped[rows - 1 : rows], (8, LANES)), 0.0
    )
    decay_all[me] = decay_out[...]

    def rim_copies():
        target = {"seq": lax.rem(me + 1, n)}
        return [
            pltpu.make_async_remote_copy(
                src_ref=src.at[pl.ds(rows - RIM, RIM)],
                dst_ref=dst,
                send_sem=rim_send.at[i],
                recv_sem=rim_recv.at[i],
                device_id=target,
                device_id_type=MESH,
            )
            for i, (src, dst) in enumerate(((x_hbm, rim_x), (state_in, rim_s)))
        ]

    spread[...] = jnp.where(
        lax.broadcasted_iota(jnp.int32, (LANES, inner), 0) % GROUP
        == lax.broadcasted_iota(jnp.int32, (LANES, inner), 1) // HEAD_DIM,
        1.0,
        0.0,
    ).astype(bf16)

    s_pad[0:RIM] = jnp.zeros((RIM, s_pad.shape[1]), f32)
    s_pad[RIM:] = state_in[...].astype(f32)
    s_conv[...] = conv_rows(s_pad, taps_s, bias_s, 0, rows, slice(None)).astype(bf16)
    x_pad[0:RIM] = jnp.zeros((RIM, inner), f32)
    load_x.wait()
    for i in range(tiles):
        c = slice(i * LANES, (i + 1) * LANES)
        x_pad[RIM:, c] = x_in[:, c].astype(f32)
        x_conv[:, c] = conv_rows(
            x_pad, taps_x[:, c], bias_x[i : i + 1], 0, rows, c
        ).astype(bf16)

    pl.semaphore_wait(barrier, n)

    @pl.when(me < n - 1)
    def _():
        for copy in rim_copies():
            copy.start()

    def decay_copy(k):
        to = lax.rem(me + k, n)
        return pltpu.make_async_remote_copy(
            src_ref=decay_out,
            dst_ref=decay_all.at[me],
            send_sem=d_send.at[k],
            recv_sem=d_recv.at[me],
            device_id={"seq": to},
            device_id_type=MESH,
        )

    def decay_start(k, _):
        decay_copy(k).start()
        return 0

    lax.fori_loop(1, n, decay_start, 0)

    load_g.wait()
    carry_decay = jnp.where(lane == 2, cols[...], 0.0)
    for i in range(tiles):
        c = slice(i * LANES, (i + 1) * LANES)
        gate_act[:, c] = silu(gate_in[:, c].astype(f32))
        decayed[:, c] = spread_heads(carry_decay, spread[:, c])

    @pl.when(me > 0)
    def _():
        for copy in rim_copies():
            copy.wait_recv()
        s_pad[0:RIM] = rim_s[...].astype(f32)
        x_pad[0:RIM] = rim_x[...].astype(f32)

    s_conv[0:16] = conv_rows(s_pad, taps_s, bias_s, 0, 16, slice(None)).astype(bf16)
    for i in range(tiles):
        c = slice(i * LANES, (i + 1) * LANES)
        x_conv[0:16, c] = conv_rows(
            x_pad, taps_x[:, c], bias_x[i : i + 1], 0, 16, c
        ).astype(bf16)

    towards = jnp.where(lane == 1, cols[...], 0.0)
    for i in range(tiles):
        c = slice(i * LANES, (i + 1) * LANES)
        scaled = (
            x_conv[:, c].astype(f32) * spread_heads(towards, spread[:, c])
        ).astype(bf16)
        full[:, c] = lax.dot_general(
            s_conv[:, :NSTATE], scaled, (((0,), (0,)), ((), ())),
            preferred_element_type=f32,
        )

    def cut(j, _):
        piece = full[pl.ds(pl.multiple_of(j * per, per), per), :]
        slices[j] = jnp.broadcast_to(piece, (slot, inner)).astype(bf16)
        return 0

    lax.fori_loop(0, n, cut, 0)

    def state_copy(k):
        to = lax.rem(me + k, n)
        return pltpu.make_async_remote_copy(
            src_ref=slices.at[to],
            dst_ref=got1.at[me],
            send_sem=s1_send.at[k],
            recv_sem=s1_recv.at[me],
            device_id={"seq": to},
            device_id_type=MESH,
        )

    @pl.when(me < n - 1)
    def _():
        def start(k, _):
            state_copy(k).start()
            return 0

        lax.fori_loop(1, n, start, 0)

    got1[me] = slices[me]

    def decay_wait(k, _):
        source = lax.rem(me + k, n)
        pltpu.make_async_remote_copy(
            src_ref=decay_out,
            dst_ref=decay_all.at[source],
            send_sem=d_send.at[k],
            recv_sem=d_recv.at[source],
            device_id={"seq": source},
            device_id_type=MESH,
        ).wait_recv()
        return 0

    lax.fori_loop(1, n, decay_wait, 0)
    decay_cols[...] = spread_heads(
        decay_all[...].reshape(n * 8, LANES), spread[...]
    ).reshape(n, 8, inner)

    keys = s_conv[:, :NSTATE]
    query = s_conv[:, NSTATE:]
    causal = (
        lax.broadcasted_iota(jnp.int32, (rows, rows), 0)
        >= lax.broadcasted_iota(jnp.int32, (rows, rows), 1)
    )
    scores[...] = jnp.where(
        causal,
        lax.dot_general(
            query, keys, (((1,), (1,)), ((), ())), preferred_element_type=f32
        ),
        0.0,
    )
    first_half = lax.broadcasted_iota(jnp.int32, (1, LANES), 1) < HEAD_DIM

    def inside(i):
        c = slice(i * LANES, (i + 1) * LANES)
        x_c = x_conv[:, c]
        tops, bottoms = [], []
        for h in (2 * i, 2 * i + 1):
            a_row = shifted[h : h + 1, :]
            top = cols[0:half, h : h + 1] - a_row[:, :half]
            top = scores[0:half, 0:half] * jnp.exp(jnp.minimum(top, 80.0))
            tops.append(
                jnp.dot(top.astype(bf16), x_c[:half], preferred_element_type=f32)
            )
            low = cols[half:, h : h + 1] - a_row
            low = scores[half:, :] * jnp.exp(jnp.minimum(low, 80.0))
            bottoms.append(jnp.dot(low.astype(bf16), x_c, preferred_element_type=f32))
        gain = jnp.where(
            first_half,
            skip_gain[:, 2 * i : 2 * i + 1],
            skip_gain[:, 2 * i + 1 : 2 * i + 2],
        )
        x_f = x_c.astype(f32)
        mixed[0:half, c] = jnp.where(first_half, *tops) + gain * x_f[:half]
        mixed[half:, c] = jnp.where(first_half, *bottoms) + gain * x_f[half:]

    split = (tiles * 6) // 10
    for i in range(split):
        inside(i)

    state = jnp.zeros((slot, inner), f32)

    def prefix(j, state):
        back[j] = state.astype(bf16)

        @pl.when(j != me)
        def _():
            pltpu.make_async_remote_copy(
                src_ref=slices.at[j],
                dst_ref=got1.at[j],
                send_sem=s1_send.at[0],
                recv_sem=s1_recv.at[j],
                device_id={"seq": lax.rem(me + 1, n)},
                device_id_type=MESH,
            ).wait_recv()

        return decay_cols[j][0:1] * state + got1[j].astype(f32)

    state = lax.fori_loop(0, n - 1, prefix, state)
    back[n - 1] = state.astype(bf16)

    def back_copy(k):
        to = lax.rem(me + k, n)
        return to, pltpu.make_async_remote_copy(
            src_ref=back.at[to],
            dst_ref=got2.at[me],
            send_sem=s2_send.at[k],
            recv_sem=s2_recv.at[me],
            device_id={"seq": to},
            device_id_type=MESH,
        )

    def back_start(k, _):
        to, copy = back_copy(k)

        @pl.when(to > 0)
        def _():
            copy.start()

        return 0

    lax.fori_loop(1, n, back_start, 0)
    got2[me] = back[me]

    for i in range(split, tiles):
        inside(i)

    @pl.when(me > 0)
    def _():
        def back_wait(k, _):
            source = lax.rem(me + k, n)
            pltpu.make_async_remote_copy(
                src_ref=back.at[source],
                dst_ref=got2.at[source],
                send_sem=s2_send.at[k],
                recv_sem=s2_recv.at[source],
                device_id={"seq": source},
                device_id_type=MESH,
            ).wait_recv()
            return 0

        lax.fori_loop(1, n, back_wait, 0)

        def place(j, _):
            entering[pl.ds(pl.multiple_of(j * per, per), per), :] = got2[j].astype(
                f32
            )[0:per]
            return 0

        lax.fori_loop(0, n, place, 0)

    @pl.when(me == 0)
    def _():
        entering[...] = jnp.zeros_like(entering)

    total = jnp.zeros((rows, LANES), f32)
    for i in range(tiles):
        c = slice(i * LANES, (i + 1) * LANES)
        carried = jnp.dot(
            query, entering[:, c].astype(bf16), preferred_element_type=f32
        )
        raw = (mixed[:, c] + carried * decayed[:, c]) * gate_act[:, c]
        total = total + raw * raw
        gated[:, c] = (raw * norm_gain[i : i + 1]).astype(bf16)
    squares[...] = total

    def across(src, dst, send, recv):
        return pltpu.make_async_remote_copy(
            src_ref=src,
            dst_ref=dst,
            send_sem=send,
            recv_sem=recv,
            device_id={"tp": other},
            device_id_type=MESH,
        )

    copy_q = across(squares, squares_got, q_sem.at[0], q_sem.at[1])
    copy_q.start()
    load_w.wait()
    pieces, _, width = part.shape

    def part_copy(p):
        return across(part.at[p], part_got.at[p], o_send.at[p], o_recv.at[p])

    for p in range(pieces):
        at = pl.ds(pl.multiple_of(other * inner + p * width, LANES), width)
        part[p] = jnp.dot(
            gated[...], w_all[:, at], preferred_element_type=f32
        ).astype(bf16)
        part_copy(p).start()
    for p in range(pieces):
        at = pl.ds(pl.multiple_of(core * inner + p * width, LANES), width)
        own[p] = jnp.dot(gated[...], w_all[:, at], preferred_element_type=f32)
    copy_q.wait_recv()
    both = jnp.sum(squares[...] + squares_got[...], axis=1, keepdims=True)
    scale = lax.rsqrt(both / (2 * inner) + 1e-05)
    for p in range(pieces):
        part_copy(p).wait_recv()
        out_ref[:, p * width : (p + 1) * width] = (
            (own[p] + part_got[p].astype(f32)) * scale
        ).astype(bf16)

    copy_q.wait_send()
    for p in range(pieces):
        part_copy(p).wait_send()

    def drain(k, _):
        decay_copy(k).wait_send()
        to, copy = back_copy(k)

        @pl.when(to > 0)
        def _():
            copy.wait_send()

        return 0

    lax.fori_loop(1, n, drain, 0)

    @pl.when(me < n - 1)
    def _():
        for copy in rim_copies():
            copy.wait_send()

        def drain1(k, _):
            state_copy(k).wait_send()
            return 0

        lax.fori_loop(1, n, drain1, 0)


def local(
    inner_input, gate_input, state_input, step_raw, conv_inner, conv_state,
    bias_inner, bias_state, step_bias, decay_log, skip_gain, norm_gain, out_weight,
):
    n = lax.axis_size("seq")
    rows, inner = inner_input.shape
    maps = state_input.shape[1]
    slot = max(8, NSTATE // n)
    width = 256
    pieces = inner // width
    vm = pltpu.VMEM
    dma = pltpu.SemaphoreType.DMA
    any_spec = pl.BlockSpec(memory_space=pltpu.HBM)
    vmem_spec = pl.BlockSpec(memory_space=pltpu.VMEM)
    scratch = [
        vm((rows, inner), bf16),
        vm((rows, inner), bf16),
        vm(out_weight.shape, bf16),
        vm((rows + RIM, inner), f32),
        vm((rows + RIM, maps), f32),
        vm((rows, inner), bf16),
        vm((rows, maps), bf16),
        vm((LANES, rows), f32),
        vm((LANES, inner), bf16),
        vm((rows, LANES), f32),
        vm((rows, rows), f32),
        vm((rows, inner), f32),
        vm((rows, inner), f32),
        vm((rows, inner), f32),
        vm((rows, inner), bf16),
        vm((RIM, inner), bf16),
        vm((RIM, maps), bf16),
        vm((8, LANES), f32),
        vm((n, 8, LANES), f32),
        vm((n, 8, inner), f32),
        vm((NSTATE, inner), f32),
        vm((n, slot, inner), bf16),
        vm((n, slot, inner), bf16),
        vm((n, slot, inner), bf16),
        vm((n, slot, inner), bf16),
        vm((NSTATE, inner), f32),
        vm((pieces, rows, width), bf16),
        vm((pieces, rows, width), bf16),
        vm((pieces, rows, width), f32),
        vm((rows, LANES), f32),
        vm((rows, LANES), f32),
        dma((3,)), dma((2,)), dma((2,)),
        dma((n,)), dma((n,)), dma((n,)), dma((n,)), dma((n,)), dma((n,)),
        dma((pieces,)), dma((pieces,)), dma((2,)),
    ]
    row = lambda v: v.reshape(1, -1)
    tile = lambda v: v.reshape(-1, LANES)
    return pl.pallas_call(
        functools.partial(kernel, n),
        out_shape=jax.ShapeDtypeStruct((rows, inner), bf16),
        in_specs=[any_spec, any_spec] + [vmem_spec] * 10 + [any_spec],
        out_specs=vmem_spec,
        scratch_shapes=scratch,
        compiler_params=pltpu.CompilerParams(
            collective_id=0, has_side_effects=True, vmem_limit_bytes=58 * 2**20
        ),
        name="ssd_block",
    )(
        inner_input, gate_input, state_input, step_raw, conv_inner, conv_state,
        tile(bias_inner), row(bias_state), row(step_bias), row(decay_log),
        row(skip_gain), tile(norm_gain), out_weight,
    )


def solution(mesh):
    return jax.shard_map(
        local,
        mesh=mesh,
        in_specs=(
            P("seq", "tp"),
            P("seq", "tp"),
            P("seq", None),
            P("tp", "seq"),
            P(None, "tp"),
            P(),
            P("tp"),
            P(),
            P("tp"),
            P("tp"),
            P("tp"),
            P("tp"),
            P("tp", None),
        ),
        out_specs=P("seq", "tp"),
        check_vma=False,
    )
```

```python
import functools

import jax
import jax.numpy as jnp
from jax import lax
from jax.experimental import pallas as pl
from jax.experimental.pallas import tpu as pltpu
from jax.sharding import PartitionSpec as P

HEAD_DIM = 64
NSTATE = 128
LANES = 128
GROUP = 32
RIM = 8
MESH = pl.DeviceIdType.MESH
f32 = jnp.float32
bf16 = jnp.bfloat16


def silu(v):
    return v / (1.0 + jnp.exp(-v))


def log1p_exp(v):
    u = jnp.exp(-jnp.abs(v))
    z = u / (2.0 + u)
    q = z * z
    series = jnp.full_like(q, 1.0 / 19.0)
    for odd in range(17, 0, -2):
        series = series * q + 1.0 / odd
    return jnp.maximum(v, 0.0) + 2.0 * z * series


def spread_heads(table, ones):
    high = table.astype(bf16)
    low = (table - high.astype(f32)).astype(bf16)
    out = jnp.dot(high, ones, preferred_element_type=f32)
    return out + jnp.dot(low, ones, preferred_element_type=f32)


def conv_rows(src, taps, bias, start, rows, columns):
    count = taps.shape[0]
    total = bias[...]
    for k in range(count):
        first = start + RIM - count + 1 + k
        total = total + taps[k : k + 1] * src[pl.ds(first, rows), columns]
    return silu(total)


def kernel(
    n,
    x_hbm, gate_hbm, state_in, step_raw, taps_x, taps_s, bias_x, bias_s,
    step_bias, decay_log, skip_gain, norm_gain, w_hbm,
    out_ref,
    x_in, gate_in, w_all, x_pad, s_pad, x_conv, s_conv, table, spread, cols,
    scores, mixed, gate_act, decayed, gated,
    rim_x, rim_s, decay_out, decay_all, decay_cols,
    full, slices, got1, back, got2, entering,
    part, part_got, own, squares, squares_got,
    load_sem, rim_send, rim_recv, d_send, d_recv, s1_send, s1_recv,
    s2_send, s2_recv, o_send, o_recv, q_sem,
):
    me = lax.axis_index("seq")
    core = lax.axis_index("tp")
    other = 1 - core
    rows, inner = x_in.shape
    heads = step_raw.shape[0]
    tiles = inner // LANES
    per = NSTATE // n
    slot = slices.shape[2]
    wide = inner // 2
    half = rows // 2

    barrier = pltpu.get_barrier_semaphore()

    def greet(k, _):
        pl.semaphore_signal(
            barrier, inc=1, device_id={"seq": lax.rem(me + k, n)}, device_id_type=MESH
        )
        return 0

    lax.fori_loop(1, n, greet, 0)
    pl.semaphore_signal(barrier, inc=1, device_id={"tp": other}, device_id_type=MESH)

    load_x = pltpu.make_async_copy(x_hbm, x_in, load_sem.at[0])
    load_g = pltpu.make_async_copy(gate_hbm, gate_in, load_sem.at[1])
    load_w = pltpu.make_async_copy(w_hbm, w_all, load_sem.at[2])
    load_x.start()
    load_g.start()
    load_w.start()

    eye = (
        lax.broadcasted_iota(jnp.int32, (heads, heads), 0)
        == lax.broadcasted_iota(jnp.int32, (heads, heads), 1)
    )

    def as_column(row):
        return jnp.sum(jnp.where(eye, row[...], 0.0), axis=1, keepdims=True)

    step = log1p_exp(step_raw[...] + as_column(step_bias))
    log_decay = -jnp.exp(as_column(decay_log)) * step
    upper = (
        lax.broadcasted_iota(jnp.int32, (rows, rows), 0)
        <= lax.broadcasted_iota(jnp.int32, (rows, rows), 1)
    ).astype(f32)
    cum = jnp.dot(
        log_decay, upper, precision=lax.Precision.HIGHEST, preferred_element_type=f32
    )
    shifted = cum - jnp.log(step)
    table[...] = jnp.zeros_like(table)
    table[0:heads] = cum
    table[GROUP : GROUP + heads] = jnp.exp(cum[:, rows - 1 : rows] - shifted)
    table[2 * GROUP : 2 * GROUP + heads] = jnp.exp(cum)
    flipped = table[...].T
    cols[...] = flipped
    lane = lax.broadcasted_iota(jnp.int32, (1, LANES), 1) // GROUP
    decay_out[...] = jnp.where(
        lane == 2, jnp.broadcast_to(flipped[rows - 1 : rows], (8, LANES)), 0.0
    )
    decay_all[me] = decay_out[...]

    def rim_copies():
        target = {"seq": lax.rem(me + 1, n)}
        return [
            pltpu.make_async_remote_copy(
                src_ref=src.at[pl.ds(rows - RIM, RIM)],
                dst_ref=dst,
                send_sem=rim_send.at[i],
                recv_sem=rim_recv.at[i],
                device_id=target,
                device_id_type=MESH,
            )
            for i, (src, dst) in enumerate(((x_hbm, rim_x), (state_in, rim_s)))
        ]

    spread[...] = jnp.where(
        lax.broadcasted_iota(jnp.int32, (LANES, inner), 0) % GROUP
        == lax.broadcasted_iota(jnp.int32, (LANES, inner), 1) // HEAD_DIM,
        1.0,
        0.0,
    ).astype(bf16)

    s_pad[0:RIM] = jnp.zeros((RIM, s_pad.shape[1]), f32)
    s_pad[RIM:] = state_in[...].astype(f32)
    s_conv[...] = conv_rows(s_pad, taps_s, bias_s, 0, rows, slice(None)).astype(bf16)
    x_pad[0:RIM] = jnp.zeros((RIM, inner), f32)
    load_x.wait()
    for i in range(tiles):
        c = slice(i * LANES, (i + 1) * LANES)
        x_pad[RIM:, c] = x_in[:, c].astype(f32)
        x_conv[:, c] = conv_rows(
            x_pad, taps_x[:, c], bias_x[i : i + 1], 0, rows, c
        ).astype(bf16)

    pl.semaphore_wait(barrier, n)

    @pl.when(me < n - 1)
    def _():
        for copy in rim_copies():
            copy.start()

    def decay_copy(k):
        to = lax.rem(me + k, n)
        return pltpu.make_async_remote_copy(
            src_ref=decay_out,
            dst_ref=decay_all.at[me],
            send_sem=d_send.at[k],
            recv_sem=d_recv.at[me],
            device_id={"seq": to},
            device_id_type=MESH,
        )

    def decay_start(k, _):
        decay_copy(k).start()
        return 0

    lax.fori_loop(1, n, decay_start, 0)

    load_g.wait()
    carry_decay = jnp.where(lane == 2, cols[...], 0.0)
    for i in range(tiles):
        c = slice(i * LANES, (i + 1) * LANES)
        gate_act[:, c] = silu(gate_in[:, c].astype(f32))
        decayed[:, c] = spread_heads(carry_decay, spread[:, c])

    @pl.when(me > 0)
    def _():
        for copy in rim_copies():
            copy.wait_recv()
        s_pad[0:RIM] = rim_s[...].astype(f32)
        x_pad[0:RIM] = rim_x[...].astype(f32)

    s_conv[0:16] = conv_rows(s_pad, taps_s, bias_s, 0, 16, slice(None)).astype(bf16)
    for i in range(tiles):
        c = slice(i * LANES, (i + 1) * LANES)
        x_conv[0:16, c] = conv_rows(
            x_pad, taps_x[:, c], bias_x[i : i + 1], 0, 16, c
        ).astype(bf16)

    def state_copy(part_no, k):
        to = lax.rem(me + k, n)
        return pltpu.make_async_remote_copy(
            src_ref=slices.at[part_no, to],
            dst_ref=got1.at[part_no, me],
            send_sem=s1_send.at[part_no, k],
            recv_sem=s1_recv.at[part_no, me],
            device_id={"seq": to},
            device_id_type=MESH,
        )

    towards = jnp.where(lane == 1, cols[...], 0.0)
    for b in range(2):
        for i in range(b * tiles // 2, (b + 1) * tiles // 2):
            c = slice(i * LANES, (i + 1) * LANES)
            scaled = (
                x_conv[:, c].astype(f32) * spread_heads(towards, spread[:, c])
            ).astype(bf16)
            full[:, c] = lax.dot_general(
                s_conv[:, :NSTATE], scaled, (((0,), (0,)), ((), ())),
                preferred_element_type=f32,
            )

        def cut(j, _, b=b):
            piece = full[
                pl.ds(pl.multiple_of(j * per, per), per), b * wide : (b + 1) * wide
            ]
            slices[b, j] = jnp.broadcast_to(piece, (slot, wide)).astype(bf16)
            return 0

        lax.fori_loop(0, n, cut, 0)

        @pl.when(me < n - 1)
        def _(b=b):
            def start(k, _):
                state_copy(b, k).start()
                return 0

            lax.fori_loop(1, n, start, 0)

        got1[b, me] = slices[b, me]

    def decay_wait(k, _):
        source = lax.rem(me + k, n)
        pltpu.make_async_remote_copy(
            src_ref=decay_out,
            dst_ref=decay_all.at[source],
            send_sem=d_send.at[k],
            recv_sem=d_recv.at[source],
            device_id={"seq": source},
            device_id_type=MESH,
        ).wait_recv()
        return 0

    lax.fori_loop(1, n, decay_wait, 0)
    decay_cols[...] = spread_heads(
        decay_all[...].reshape(n * 8, LANES), spread[...]
    ).reshape(n, 8, inner)

    keys = s_conv[:, :NSTATE]
    query = s_conv[:, NSTATE:]
    causal = (
        lax.broadcasted_iota(jnp.int32, (rows, rows), 0)
        >= lax.broadcasted_iota(jnp.int32, (rows, rows), 1)
    )
    scores[...] = jnp.where(
        causal,
        lax.dot_general(
            query, keys, (((1,), (1,)), ((), ())), preferred_element_type=f32
        ),
        0.0,
    )
    first_half = lax.broadcasted_iota(jnp.int32, (1, LANES), 1) < HEAD_DIM

    def inside(i):
        c = slice(i * LANES, (i + 1) * LANES)
        x_c = x_conv[:, c]
        tops, bottoms = [], []
        for h in (2 * i, 2 * i + 1):
            a_row = shifted[h : h + 1, :]
            top = cols[0:half, h : h + 1] - a_row[:, :half]
            top = scores[0:half, 0:half] * jnp.exp(jnp.minimum(top, 80.0))
            tops.append(
                jnp.dot(top.astype(bf16), x_c[:half], preferred_element_type=f32)
            )
            low = cols[half:, h : h + 1] - a_row
            low = scores[half:, :] * jnp.exp(jnp.minimum(low, 80.0))
            bottoms.append(jnp.dot(low.astype(bf16), x_c, preferred_element_type=f32))
        gain = jnp.where(
            first_half,
            skip_gain[:, 2 * i : 2 * i + 1],
            skip_gain[:, 2 * i + 1 : 2 * i + 2],
        )
        x_f = x_c.astype(f32)
        mixed[0:half, c] = jnp.where(first_half, *tops) + gain * x_f[:half]
        mixed[half:, c] = jnp.where(first_half, *bottoms) + gain * x_f[half:]

    for i in range(tiles):
        inside(i)

    def back_copy(b, k):
        to = lax.rem(me + k, n)
        return to, pltpu.make_async_remote_copy(
            src_ref=back.at[b, to],
            dst_ref=got2.at[b, me],
            send_sem=s2_send.at[b, k],
            recv_sem=s2_recv.at[b, me],
            device_id={"seq": to},
            device_id_type=MESH,
        )

    for b in range(2):
        c = slice(b * wide, (b + 1) * wide)

        def prefix(j, state, b=b, c=c):
            back[b, j] = state.astype(bf16)

            @pl.when(j != me)
            def _():
                pltpu.make_async_remote_copy(
                    src_ref=slices.at[b, j],
                    dst_ref=got1.at[b, j],
                    send_sem=s1_send.at[b, 0],
                    recv_sem=s1_recv.at[b, j],
                    device_id={"seq": lax.rem(me + 1, n)},
                    device_id_type=MESH,
                ).wait_recv()

            return decay_cols[j][0:1, c] * state + got1[b, j].astype(f32)

        state = lax.fori_loop(0, n - 1, prefix, jnp.zeros((slot, wide), f32))
        back[b, n - 1] = state.astype(bf16)

        def back_start(k, _, b=b):
            to, copy = back_copy(b, k)

            @pl.when(to > 0)
            def _():
                copy.start()

            return 0

        lax.fori_loop(1, n, back_start, 0)
        got2[b, me] = back[b, me]

    @pl.when(me > 0)
    def _():
        for b in range(2):

            def back_wait(k, _, b=b):
                source = lax.rem(me + k, n)
                pltpu.make_async_remote_copy(
                    src_ref=back.at[b, source],
                    dst_ref=got2.at[b, source],
                    send_sem=s2_send.at[b, k],
                    recv_sem=s2_recv.at[b, source],
                    device_id={"seq": source},
                    device_id_type=MESH,
                ).wait_recv()
                return 0

            lax.fori_loop(1, n, back_wait, 0)

            def place(j, _, b=b):
                entering[
                    pl.ds(pl.multiple_of(j * per, per), per), b * wide : (b + 1) * wide
                ] = got2[b, j].astype(f32)[0:per]
                return 0

            lax.fori_loop(0, n, place, 0)

    @pl.when(me == 0)
    def _():
        entering[...] = jnp.zeros_like(entering)

    total = jnp.zeros((rows, LANES), f32)
    for i in range(tiles):
        c = slice(i * LANES, (i + 1) * LANES)
        carried = jnp.dot(
            query, entering[:, c].astype(bf16), preferred_element_type=f32
        )
        raw = (mixed[:, c] + carried * decayed[:, c]) * gate_act[:, c]
        total = total + raw * raw
        gated[:, c] = (raw * norm_gain[i : i + 1]).astype(bf16)
    squares[...] = total

    def across(src, dst, send, recv):
        return pltpu.make_async_remote_copy(
            src_ref=src,
            dst_ref=dst,
            send_sem=send,
            recv_sem=recv,
            device_id={"tp": other},
            device_id_type=MESH,
        )

    copy_q = across(squares, squares_got, q_sem.at[0], q_sem.at[1])
    copy_q.start()
    load_w.wait()
    pieces, _, width = part.shape

    def part_copy(p):
        return across(part.at[p], part_got.at[p], o_send.at[p], o_recv.at[p])

    for p in range(pieces):
        at = pl.ds(pl.multiple_of(other * inner + p * width, LANES), width)
        part[p] = jnp.dot(
            gated[...], w_all[:, at], preferred_element_type=f32
        ).astype(bf16)
        part_copy(p).start()
    for p in range(pieces):
        at = pl.ds(pl.multiple_of(core * inner + p * width, LANES), width)
        own[p] = jnp.dot(gated[...], w_all[:, at], preferred_element_type=f32)
    copy_q.wait_recv()
    both = jnp.sum(squares[...] + squares_got[...], axis=1, keepdims=True)
    scale = lax.rsqrt(both / (2 * inner) + 1e-05)
    for p in range(pieces):
        part_copy(p).wait_recv()
        out_ref[:, p * width : (p + 1) * width] = (
            (own[p] + part_got[p].astype(f32)) * scale
        ).astype(bf16)

    copy_q.wait_send()
    for p in range(pieces):
        part_copy(p).wait_send()

    def drain(k, _):
        decay_copy(k).wait_send()
        for b in range(2):
            to, copy = back_copy(b, k)

            @pl.when(to > 0)
            def _(copy=copy):
                copy.wait_send()

        return 0

    lax.fori_loop(1, n, drain, 0)

    @pl.when(me < n - 1)
    def _():
        for copy in rim_copies():
            copy.wait_send()

        def drain1(k, _):
            state_copy(0, k).wait_send()
            state_copy(1, k).wait_send()
            return 0

        lax.fori_loop(1, n, drain1, 0)


def local(
    inner_input, gate_input, state_input, step_raw, conv_inner, conv_state,
    bias_inner, bias_state, step_bias, decay_log, skip_gain, norm_gain, out_weight,
):
    n = lax.axis_size("seq")
    rows, inner = inner_input.shape
    maps = state_input.shape[1]
    slot = max(8, NSTATE // n)
    width = 256
    pieces = inner // width
    vm = pltpu.VMEM
    dma = pltpu.SemaphoreType.DMA
    any_spec = pl.BlockSpec(memory_space=pltpu.HBM)
    vmem_spec = pl.BlockSpec(memory_space=pltpu.VMEM)
    scratch = [
        vm((rows, inner), bf16),
        vm((rows, inner), bf16),
        vm(out_weight.shape, bf16),
        vm((rows + RIM, inner), f32),
        vm((rows + RIM, maps), f32),
        vm((rows, inner), bf16),
        vm((rows, maps), bf16),
        vm((LANES, rows), f32),
        vm((LANES, inner), bf16),
        vm((rows, LANES), f32),
        vm((rows, rows), f32),
        vm((rows, inner), f32),
        vm((rows, inner), f32),
        vm((rows, inner), f32),
        vm((rows, inner), bf16),
        vm((RIM, inner), bf16),
        vm((RIM, maps), bf16),
        vm((8, LANES), f32),
        vm((n, 8, LANES), f32),
        vm((n, 8, inner), f32),
        vm((NSTATE, inner), f32),
        vm((2, n, slot, inner // 2), bf16),
        vm((2, n, slot, inner // 2), bf16),
        vm((2, n, slot, inner // 2), bf16),
        vm((2, n, slot, inner // 2), bf16),
        vm((NSTATE, inner), f32),
        vm((pieces, rows, width), bf16),
        vm((pieces, rows, width), bf16),
        vm((pieces, rows, width), f32),
        vm((rows, LANES), f32),
        vm((rows, LANES), f32),
        dma((3,)), dma((2,)), dma((2,)),
        dma((n,)), dma((n,)), dma((2, n)), dma((2, n)), dma((2, n)), dma((2, n)),
        dma((pieces,)), dma((pieces,)), dma((2,)),
    ]
    row = lambda v: v.reshape(1, -1)
    tile = lambda v: v.reshape(-1, LANES)
    return pl.pallas_call(
        functools.partial(kernel, n),
        out_shape=jax.ShapeDtypeStruct((rows, inner), bf16),
        in_specs=[any_spec, any_spec] + [vmem_spec] * 10 + [any_spec],
        out_specs=vmem_spec,
        scratch_shapes=scratch,
        compiler_params=pltpu.CompilerParams(
            collective_id=0, has_side_effects=True, vmem_limit_bytes=58 * 2**20
        ),
        name="ssd_block",
    )(
        inner_input, gate_input, state_input, step_raw, conv_inner, conv_state,
        tile(bias_inner), row(bias_state), row(step_bias), row(decay_log),
        row(skip_gain), tile(norm_gain), out_weight,
    )


def solution(mesh):
    return jax.shard_map(
        local,
        mesh=mesh,
        in_specs=(
            P("seq", "tp"),
            P("seq", "tp"),
            P("seq", None),
            P("tp", "seq"),
            P(None, "tp"),
            P(),
            P("tp"),
            P(),
            P("tp"),
            P("tp"),
            P("tp"),
            P("tp"),
            P("tp", None),
        ),
        out_specs=P("seq", "tp"),
        check_vma=False,
    )
```
